16 devices in a mesh: dpz: 2 (over z), dpy: 2 (over y), dpx: 4 (over x, core).
Axes of the slice: x: 2, y: 2, z: 2, core: 2. Of those that a mesh axis runs over, the one named last changes fastest.
Arguments:
- x_in: bfloat16 [65536, 768], P(('dpz', 'dpy', 'dpx'))
- dy_out: bfloat16 [65536, 768], P(('dpz', 'dpy', 'dpx'))
- w1_in: bfloat16 [768, 3072], replicated
- w1_out: bfloat16 [3072, 768], replicated
- w2_in: bfloat16 [768, 3072], replicated
- w2_out: bfloat16 [3072, 768], replicated
- master: float32 [9437184], P(('dpz', 'dpy', 'dpx'))
- adam_m: float32 [9437184], P(('dpz', 'dpy', 'dpx'))
- adam_v: float32 [9437184], P(('dpz', 'dpy', 'dpx'))
Outputs:
- output 1: float32 [9437184], P(('dpz', 'dpy', 'dpx'))
- output 2: float32 [9437184], P(('dpz', 'dpy', 'dpx'))
- output 3: float32 [9437184], P(('dpz', 'dpy', 'dpx'))
- output 4: bfloat16 [9437184], replicated
All inputs are finite; a program needn't handle non-finite values.
Results may differ from the reference program's by a relative error of at most 0.00931221.
Values are sent between devices in bfloat16 or wider.
A program may use at most 1 GiB of HBM per device.

```python
import math
import jax
import jax.numpy as jnp
from jax import lax

D = 768
FF = 3072
TOKENS = 4096
NDEV = 16
STEP = 10

BETA_ONE = 0.9
BETA_TWO = 0.999
LEARN_RATE = 0.001
ADAM_EPS = 1e-8


def gelu_value(z_val):
    return 0.5 * z_val * (1.0 + lax.erf(z_val * (1.0 / math.sqrt(2.0))))


def gelu_slope(z_val):
    cdf_part = 0.5 * (1.0 + lax.erf(z_val * (1.0 / math.sqrt(2.0))))
    return cdf_part + z_val * jnp.exp(-0.5 * z_val * z_val) * (1.0 / math.sqrt(2.0 * math.pi))


def setup_inputs(seed: int = 0) -> dict:
    key_list = jax.random.split(jax.random.key(seed), 9)
    total_len = 4 * D * FF
    row_count = NDEV * TOKENS
    grad_scale = math.sqrt(row_count)
    act_vals = jax.random.normal(key_list[0], (row_count, D), jnp.float32)
    out_grad = jax.random.normal(key_list[1], (row_count, D), jnp.float32)
    w1_in = jax.random.normal(key_list[2], (D, FF), jnp.float32) * D ** -0.5
    w1_out = jax.random.normal(key_list[3], (FF, D), jnp.float32) * FF ** -0.5
    w2_in = jax.random.normal(key_list[4], (D, FF), jnp.float32) * D ** -0.5
    w2_out = jax.random.normal(key_list[5], (FF, D), jnp.float32) * FF ** -0.5
    master = jax.random.normal(key_list[6], (total_len,), jnp.float32) * 0.02
    adam_m = jax.random.normal(key_list[7], (total_len,), jnp.float32) * (0.05 * grad_scale)
    adam_v = jax.random.uniform(key_list[8], (total_len,), jnp.float32, 0.5, 1.5) * (0.0004 * row_count)
    return {'x_in': act_vals.astype(jnp.bfloat16), 'dy_out': out_grad.astype(jnp.bfloat16), 'w1_in': w1_in.astype(jnp.bfloat16), 'w1_out': w1_out.astype(jnp.bfloat16), 'w2_in': w2_in.astype(jnp.bfloat16), 'w2_out': w2_out.astype(jnp.bfloat16), 'master': master, 'adam_m': adam_m, 'adam_v': adam_v}


def device_grads(x_one, dy_one, w1_in, w1_out, w2_in, w2_out):
    z_one = jnp.dot(x_one, w1_in, preferred_element_type=jnp.float32).astype(jnp.bfloat16)
    h_one = gelu_value(z_one.astype(jnp.float32)).astype(jnp.bfloat16)
    x_two = (x_one.astype(jnp.float32) + jnp.dot(h_one, w1_out, preferred_element_type=jnp.float32)).astype(jnp.bfloat16)
    z_two = jnp.dot(x_two, w2_in, preferred_element_type=jnp.float32).astype(jnp.bfloat16)
    h_two = gelu_value(z_two.astype(jnp.float32)).astype(jnp.bfloat16)
    g2_out = jnp.dot(h_two.T, dy_one, preferred_element_type=jnp.float32).astype(jnp.bfloat16)
    dz_two = (jnp.dot(dy_one, w2_out.T, preferred_element_type=jnp.float32) * gelu_slope(z_two.astype(jnp.float32))).astype(jnp.bfloat16)
    g2_in = jnp.dot(x_two.T, dz_two, preferred_element_type=jnp.float32).astype(jnp.bfloat16)
    dx_two = (dy_one.astype(jnp.float32) + jnp.dot(dz_two, w2_in.T, preferred_element_type=jnp.float32)).astype(jnp.bfloat16)
    g1_out = jnp.dot(h_one.T, dx_two, preferred_element_type=jnp.float32).astype(jnp.bfloat16)
    dz_one = (jnp.dot(dx_two, w1_out.T, preferred_element_type=jnp.float32) * gelu_slope(z_one.astype(jnp.float32))).astype(jnp.bfloat16)
    g1_in = jnp.dot(x_one.T, dz_one, preferred_element_type=jnp.float32).astype(jnp.bfloat16)
    return jnp.concatenate([g2_out.reshape(-1), g2_in.reshape(-1), g1_out.reshape(-1), g1_in.reshape(-1)])


def adam_update(master, adam_m, adam_v, grad_sum):
    new_m = BETA_ONE * adam_m + (1.0 - BETA_ONE) * grad_sum
    new_v = BETA_TWO * adam_v + (1.0 - BETA_TWO) * grad_sum * grad_sum
    m_hat = new_m / (1.0 - BETA_ONE ** STEP)
    v_hat = new_v / (1.0 - BETA_TWO ** STEP)
    new_master = master - LEARN_RATE * m_hat / (jnp.sqrt(v_hat) + ADAM_EPS)
    return new_master, new_m, new_v


def reference(x_in, dy_out, w1_in, w1_out, w2_in, w2_out, master, adam_m, adam_v):
    x_dev = x_in.reshape(NDEV, TOKENS, D)
    dy_dev = dy_out.reshape(NDEV, TOKENS, D)

    def accumulate(run_sum, dev_pair):
        grads = device_grads(dev_pair[0], dev_pair[1], w1_in, w1_out, w2_in, w2_out)
        return run_sum + grads.astype(jnp.float32), None

    start_sum = jnp.zeros((4 * D * FF,), jnp.float32)
    grad_sum = lax.scan(accumulate, start_sum, (x_dev, dy_dev))[0]
    new_master, new_m, new_v = adam_update(master, adam_m, adam_v, grad_sum)
    return (new_master, new_m, new_v, new_master.astype(jnp.bfloat16))
```

```python
import math
import jax
import jax.numpy as jnp
from jax import lax
from jax.experimental import pallas as pl
from jax.experimental.pallas import tpu as pltpu
from jax.sharding import PartitionSpec as P

AXES = ('dpz', 'dpy', 'dpx')
STEP = 10
BETA_ONE = 0.9
BETA_TWO = 0.999
LEARN_RATE = 0.001
ADAM_EPS = 1e-8


def gelu_value(z_val):
    return 0.5 * z_val * (1.0 + lax.erf(z_val * (1.0 / math.sqrt(2.0))))


def gelu_slope(z_val):
    cdf_part = 0.5 * (1.0 + lax.erf(z_val * (1.0 / math.sqrt(2.0))))
    return cdf_part + z_val * jnp.exp(-0.5 * z_val * z_val) * (1.0 / math.sqrt(2.0 * math.pi))


def dev(z, y, x):
    return (z * 2 + y) * 4 + x


def send_x(blocks, x_idx):
    own = lax.dynamic_index_in_dim(blocks, x_idx, 0, keepdims=False)
    got = [own]
    for k in (2, 3, 1):
        send = lax.dynamic_index_in_dim(blocks, x_idx ^ k, 0, keepdims=False)
        got.append(lax.ppermute(send, 'dpx', [(i, i ^ k) for i in range(4)]))
    return got


def add_x(got):
    total = got[3].astype(jnp.float32) + got[0].astype(jnp.float32)
    return total + (got[1].astype(jnp.float32) + got[2].astype(jnp.float32))


def shift_z(val, y_rel, zo, yo):
    pairs = [(dev(1 - zo, yo ^ ry, x), dev(zo, yo ^ ry, x)) for ry in y_rel for x in range(4)]
    return lax.ppermute(val, AXES, pairs)


def shift_y(val, z_rel, zo, yo):
    pairs = [(dev(zo ^ rz, 1 - yo, x), dev(zo ^ rz, yo, x)) for rz in z_rel for x in range(4)]
    return lax.ppermute(val, AXES, pairs)


def send_one(part, zo, yo):
    half = part.shape[0] // 2
    a_part, b_part = part[:half], part[half:]
    return a_part, b_part, shift_z(a_part, (0, 1), zo, yo), shift_y(b_part, (0, 1), zo, yo)


def add_one(sent):
    return sent[0] + sent[2], sent[1] + sent[3]


def send_two(halves, zo, yo):
    return halves[0], halves[1], shift_y(halves[0], (0,), zo, yo), shift_z(halves[1], (0,), zo, yo)


def add_two(sent):
    return jnp.concatenate([sent[0] + sent[2], sent[1] + sent[3]], axis=0)


def after(val, *deps):
    out = lax.optimization_barrier((val,) + deps)
    return out[0], out[1:]


SHARD_ROWS = 4608
N_PIECE = 6
PIECE_ROWS = SHARD_ROWS // N_PIECE
CH_COLS = 512
N_CH = 6
N_PRE = 4
PRE_COLS = N_PRE * CH_COLS
REST_COLS = 3072 - PRE_COLS
X_BIT, Y_BIT, Z_BIT = 1, 2, 4
ADAM_ROWS = 96
ORDERS = ((X_BIT, Y_BIT, Z_BIT), (Y_BIT, Z_BIT, X_BIT), (Z_BIT, X_BIT, Y_BIT)) * 2


def tail_kernel(p_hbm, gd_hbm, s_hbm, mst_hbm, m_hbm, v_hbm,
                omst_hbm, om_hbm, ov_hbm, w_hbm,
                own, xrecv, part, a1, b1, a2, b2, s_v, mst_v, m_v, v_v, w_v,
                ld_sem, st_sem, xs_send, xs_recv, yz_send, yz_recv, ag_send, ag_recv, dd_send, dd_recv):
    z, y, x = (lax.axis_index(a) for a in AXES)
    ny, nz = 1 - y, 1 - z
    is_late = (z == 1) & (y == 1)
    f32 = jnp.float32

    def x_peer(k):
        if k == 2:
            return lax.rem(x + 2, 4)
        flip = x + 1 - 2 * lax.rem(x, 2)
        return flip if k == 1 else lax.rem(flip + 2, 4)

    peers = {X_BIT: {'dpx': x_peer(2)}, Y_BIT: {'dpy': ny}, Z_BIT: {'dpz': nz}}

    barrier = pltpu.get_barrier_semaphore()
    for where in ({'dpx': x_peer(1)}, {'dpx': x_peer(2)}, {'dpx': x_peer(3)}, {'dpy': ny}, {'dpz': nz}):
        pl.semaphore_signal(barrier, inc=1, device_id=where, device_id_type=pl.DeviceIdType.MESH)
    pl.semaphore_wait(barrier, 5)

    def remote(src, dst, send, recv, where):
        return pltpu.make_async_remote_copy(src_ref=src, dst_ref=dst, send_sem=send, recv_sem=recv,
                                            device_id=where, device_id_type=pl.DeviceIdType.MESH)

    def xs_copy(k, ch):
        lo = (ch - N_PRE) * CH_COLS
        to = x_peer(k)
        return remote(gd_hbm.at[pl.ds(to * 192, 192), pl.ds(lo, CH_COLS)],
                      xrecv.at[k - 1, :, pl.ds(lo, CH_COLS)],
                      xs_send.at[k - 1, ch - N_PRE], xs_recv.at[k - 1, ch - N_PRE], {'dpx': to})

    for ch in range(N_PRE, N_CH):
        for k in (2, 3, 1):
            xs_copy(k, ch).start()

    loads = [pltpu.make_async_copy(p_hbm, part.at[:, pl.ds(0, PRE_COLS)], ld_sem.at[0]),
             pltpu.make_async_copy(gd_hbm.at[pl.ds(x * 192, 192), :], own, ld_sem.at[1]),
             pltpu.make_async_copy(mst_hbm, mst_v, ld_sem.at[2]),
             pltpu.make_async_copy(m_hbm, m_v, ld_sem.at[3]),
             pltpu.make_async_copy(v_hbm, v_v, ld_sem.at[4])]
    for cp in loads:
        cp.start()
    load_s = pltpu.make_async_copy(s_hbm, s_v, ld_sem.at[5])

    @pl.when(jnp.logical_not(is_late))
    def _():
        load_s.start()

    loads[0].wait()

    def cols(ch):
        return pl.ds(ch * CH_COLS, CH_COLS)

    top, bot = pl.ds(0, 96), pl.ds(96, 96)

    def yz_copy(kind, ch):
        rows, dst, where = ((top, a1, peers[Z_BIT]), (bot, b1, peers[Y_BIT]),
                            (top, a2, peers[Y_BIT]), (bot, b2, peers[Z_BIT]))[kind]
        return remote(part.at[rows, cols(ch)], dst.at[:, cols(ch)],
                      yz_send.at[kind, ch], yz_recv.at[kind, ch], where)

    yz_sends = {0: z == 0, 1: y == 0, 2: (z == 1) & (y == 0), 3: (z == 0) & (y == 1)}
    yz_takes = {0: z == 1, 1: y == 1, 2: is_late, 3: is_late}

    def yz_start(kind, ch):
        @pl.when(yz_sends[kind])
        def _():
            yz_copy(kind, ch).start()

    def yz_take(kind, ch):
        @pl.when(yz_takes[kind])
        def _():
            yz_copy(kind, ch).wait_recv()
            got = (a1, b1, a2, b2)[kind]
            base = 0 if kind in (0, 2) else 96

            def body(i, _):
                rows = pl.ds(pl.multiple_of(base + i * 8, 8), 8)
                part[rows, cols(ch)] += got[pl.ds(pl.multiple_of(i * 8, 8), 8), cols(ch)]
                return 0

            lax.fori_loop(0, 12, body, 0)

    def x_sum(ch):
        lo = (ch - N_PRE) * CH_COLS
        for k in (2, 3, 1):
            xs_copy(k, ch).wait_recv()

        def body(i, _):
            rows = pl.ds(pl.multiple_of(i * 16, 16), 16)
            cc = pl.ds(lo, CH_COLS)
            part[rows, cols(ch)] = ((own[rows, cc].astype(f32) + xrecv[0, rows, cc].astype(f32))
                                    + (xrecv[1, rows, cc].astype(f32) + xrecv[2, rows, cc].astype(f32)))
            return 0

        lax.fori_loop(0, 12, body, 0)

    def adam():
        def body(i, _):
            rows = pl.ds(pl.multiple_of(i * ADAM_ROWS, ADAM_ROWS), ADAM_ROWS)
            g_sum = s_v[rows, :]
            new_m = BETA_ONE * m_v[rows, :] + (1.0 - BETA_ONE) * g_sum
            new_v = BETA_TWO * v_v[rows, :] + (1.0 - BETA_TWO) * g_sum * g_sum
            m_hat = new_m / (1.0 - BETA_ONE ** STEP)
            v_hat = new_v / (1.0 - BETA_TWO ** STEP)
            new_w = mst_v[rows, :] - LEARN_RATE * m_hat / (jnp.sqrt(v_hat) + ADAM_EPS)
            m_v[rows, :] = new_m
            v_v[rows, :] = new_v
            mst_v[rows, :] = new_w
            w_v[rows, :] = new_w.astype(jnp.bfloat16)
            return 0

        lax.fori_loop(0, SHARD_ROWS // ADAM_ROWS, body, 0)

    def shard_rows(h, r):
        zz = nz if r & Z_BIT else z
        yy = ny if r & Y_BIT else y
        xx = x_peer(2) if r & X_BIT else x
        return pl.ds(pl.multiple_of(((zz * 2 + yy) * 4 + xx) * SHARD_ROWS + h * PIECE_ROWS, 256), PIECE_ROWS)

    def ag_copy(h, r, bit):
        rows = shard_rows(h, r)
        return remote(w_hbm.at[rows, :], w_hbm.at[rows, :], ag_send.at[h, bit.bit_length() - 1, r],
                      ag_recv.at[h, r ^ bit], peers[bit])

    def ag_arrived(h, r):
        rows = shard_rows(h, r)
        bit = ORDERS[h][max(i for i in range(3) if r & ORDERS[h][i])]
        remote(w_hbm.at[rows, :], w_hbm.at[rows, :], ag_send.at[h, 0, r], ag_recv.at[h, r], peers[bit]).wait_recv()

    def dd_copy(h, r):
        rows = shard_rows(h, r)
        return remote(w_hbm.at[rows, :], w_hbm.at[rows, :], dd_send.at[h, r], dd_recv.at[h, r], {'dpx': x_peer(1)})

    def next_bits(h, r):
        last = max([i for i in range(3) if r & ORDERS[h][i]], default=-1)
        return ORDERS[h][last + 1:]

    def hops(step):
        for sub in range(1 << step):
            for h in range(N_PIECE):
                o = ORDERS[h]
                r = o[step] | (o[0] if sub & 1 else 0) | (o[1] if sub & 2 else 0)
                ag_arrived(h, r)
                for bit in next_bits(h, r):
                    ag_copy(h, r, bit).start()
                dd_copy(h, r).start()

    outs = [pltpu.make_async_copy(mst_v, omst_hbm, st_sem.at[0]),
            pltpu.make_async_copy(m_v, om_hbm, st_sem.at[1]),
            pltpu.make_async_copy(v_v, ov_hbm, st_sem.at[2])]

    def own_update():
        adam()
        mine = shard_rows(0, 0)
        rows = pl.ds(mine.start, SHARD_ROWS)
        put = pltpu.make_async_copy(w_v, w_hbm.at[rows, :], st_sem.at[3])
        put.start()
        for cp in outs:
            cp.start()
        put.wait()

    for ch in range(N_PRE):
        yz_start(0, ch)
        yz_start(1, ch)
    for cp in loads[1:]:
        cp.wait()

    @pl.when(jnp.logical_not(is_late))
    def _():
        load_s.wait()
        own_update()

    for ch in range(N_PRE):
        yz_take(0, ch)
        yz_take(1, ch)
        yz_start(2, ch)
        yz_start(3, ch)
    for ch in range(N_PRE, N_CH):
        x_sum(ch)
        yz_start(0, ch)
        yz_start(1, ch)
    for ch in range(N_PRE, N_CH):
        yz_take(0, ch)
        yz_take(1, ch)
        yz_start(2, ch)
        yz_start(3, ch)

    @pl.when(is_late)
    def _():
        for ch in range(N_CH):
            for kind in (2, 3):
                yz_take(kind, ch)

        def body(g, _):
            rows = pl.ds(pl.multiple_of(g * 8, 8), 8)
            for j in range(24):
                s_v[pl.ds(g * 192 + j, 8, stride=24), :] = part[rows, 128 * j:128 * (j + 1)]
            return 0

        lax.fori_loop(0, 24, body, 0)
        own_update()

    for step in range(3):
        for h in range(N_PIECE):
            ag_copy(h, 0, ORDERS[h][step]).start()
    for h in range(N_PIECE):
        dd_copy(h, 0).start()
    for step in range(3):
        hops(step)

    for h in range(N_PIECE):
        for r in range(8):
            for bit in next_bits(h, r):
                ag_copy(h, r, bit).wait_send()
            dd_copy(h, r).wait()
    for ch in range(N_PRE, N_CH):
        for k in (1, 2, 3):
            xs_copy(k, ch).wait_send()
    for ch in range(N_CH):
        for kind in range(4):
            @pl.when(yz_sends[kind])
            def _():
                yz_copy(kind, ch).wait_send()
    for cp in outs:
        cp.wait()


def tail(p_d0, g_d1, s_abc, master, adam_m, adam_v):
    any_spec = pl.BlockSpec(memory_space=pl.ANY)
    f32, bf16 = jnp.float32, jnp.bfloat16
    dma = pltpu.SemaphoreType.DMA
    shard = jax.ShapeDtypeStruct((SHARD_ROWS, 128), f32)
    state = pltpu.VMEM((SHARD_ROWS, 128), f32)
    return pl.pallas_call(
        tail_kernel,
        out_shape=(shard, shard, shard, jax.ShapeDtypeStruct((16 * SHARD_ROWS, 128), bf16)),
        in_specs=[any_spec] * 6,
        out_specs=[any_spec] * 4,
        scratch_shapes=[
            pltpu.VMEM((192, REST_COLS), bf16), pltpu.VMEM((3, 192, REST_COLS), bf16), pltpu.VMEM((192, 3072), f32),
            pltpu.VMEM((96, 3072), f32), pltpu.VMEM((96, 3072), f32), pltpu.VMEM((96, 3072), f32),
            pltpu.VMEM((96, 3072), f32), state, state, state, state, pltpu.VMEM((SHARD_ROWS, 128), bf16),
            dma((6,)), dma((4,)), dma((3, N_CH - N_PRE)), dma((3, N_CH - N_PRE)), dma((4, N_CH)), dma((4, N_CH)),
            dma((6, 3, 8)), dma((6, 8)), dma((6, 8)), dma((6, 8)),
        ],
        compiler_params=pltpu.CompilerParams(collective_id=0, has_side_effects=True, vmem_limit_bytes=48 << 20),
        name="tail",
    )(p_d0, g_d1, s_abc, master, adam_m, adam_v)


def solution(mesh):
    def inner_step(x_one, dy_one, w1_in, w1_out, w2_in, w2_out, master, adam_m, adam_v):
        zi, yi, xi = (lax.axis_index(a) for a in AXES)
        f32, bf16 = jnp.float32, jnp.bfloat16

        def mm(spec, a, b):
            return jnp.einsum(spec, a, b, preferred_element_type=f32)

        z_one = mm('td,df->tf', x_one, w1_in).astype(bf16)
        h_one = gelu_value(z_one.astype(f32)).astype(bf16)
        z_one, h_one = lax.optimization_barrier((z_one, h_one))
        x_two = (x_one.astype(f32) + mm('tf,fd->td', h_one, w1_out)).astype(bf16)
        z_two = mm('td,df->tf', x_two, w2_in).astype(bf16)
        h_two = gelu_value(z_two.astype(f32)).astype(bf16)
        z_two, h_two = lax.optimization_barrier((z_two, h_two))
        g_a = mm('tf,td->fd', h_two, dy_one).astype(bf16)
        x_a = send_x(g_a.reshape(4, 768, 768), xi)
        dz_two = (mm('td,fd->tf', dy_one, w2_out) * gelu_slope(z_two.astype(f32))).astype(bf16)
        g_b = mm('td,tf->df', x_two, dz_two).astype(bf16)
        x_b = send_x(g_b.reshape(4, 192, 3072), xi)
        p_a = add_x(x_a)
        dz_two, (p_a,) = after(dz_two, p_a)
        one_a = send_one(p_a, 0, 0)
        dx_two = (dy_one.astype(f32) + mm('tf,df->td', dz_two, w2_in)).astype(bf16)
        g_c = mm('tf,td->fd', h_one, dx_two).astype(bf16)
        x_c = send_x(g_c.reshape(4, 768, 768), xi)
        p_b = add_x(x_b)
        q_a = add_one(one_a)
        dx_two, (p_b, qa0, qa1) = after(dx_two, p_b, *q_a)
        two_a = send_two((qa0, qa1), 0, 0)
        one_b = send_one(p_b, 0, 1)

        def slope_grad(lo, hi):
            up = mm('td,fd->tf', dx_two, w1_out[lo:hi])
            return (up * gelu_slope(z_one[:, lo:hi].astype(f32))).astype(bf16)

        dz_pre = slope_grad(0, PRE_COLS)
        s_a = add_two(two_a).reshape(-1)
        q_b = add_one(one_b)
        dz_pre, (qb0, qb1, s_a) = after(dz_pre, *q_b, s_a)
        two_b = send_two((qb0, qb1), 0, 1)
        g_d0 = mm('td,tf->df', x_one, dz_pre).astype(bf16)
        x_d0 = send_x(g_d0.reshape(4, 192, PRE_COLS), xi)
        p_c = add_x(x_c)
        dx_two, (p_c,) = after(dx_two, p_c)
        one_c = send_one(p_c, 1, 0)
        dz_rest = slope_grad(PRE_COLS, 3072)
        s_b = add_two(two_b).reshape(-1)
        q_c = add_one(one_c)
        dz_rest, (qc0, qc1, s_b) = after(dz_rest, *q_c, s_b)
        two_c = send_two((qc0, qc1), 1, 0)
        g_d1 = mm('td,tf->df', x_one, dz_rest).astype(bf16)
        s_c = add_two(two_c).reshape(-1)
        s_abc = jnp.where(zi == 0, jnp.where(yi == 0, s_a, s_b), s_c)
        flat = lambda t: t.reshape(SHARD_ROWS, 128)
        new_master, new_m, new_v, weights = tail(add_x(x_d0), g_d1, flat(s_abc), flat(master), flat(adam_m), flat(adam_v))
        return new_master.reshape(-1), new_m.reshape(-1), new_v.reshape(-1), weights.reshape(-1)

    in_specs = (P(AXES, None), P(AXES, None), P(), P(), P(), P(), P(AXES), P(AXES), P(AXES))
    out_specs = (P(AXES), P(AXES), P(AXES), P())
    return jax.shard_map(inner_step, mesh=mesh, in_specs=in_specs, out_specs=out_specs, check_vma=False)
```

```python
import math
import jax
import jax.numpy as jnp
from jax import lax
from jax.experimental import pallas as pl
from jax.experimental.pallas import tpu as pltpu
from jax.sharding import PartitionSpec as P

AXES = ('dpz', 'dpy', 'dpx')
STEP = 10
BETA_ONE = 0.9
BETA_TWO = 0.999
LEARN_RATE = 0.001
ADAM_EPS = 1e-8


def gelu_value(z_val):
    return 0.5 * z_val * (1.0 + lax.erf(z_val * (1.0 / math.sqrt(2.0))))


def gelu_slope(z_val):
    cdf_part = 0.5 * (1.0 + lax.erf(z_val * (1.0 / math.sqrt(2.0))))
    return cdf_part + z_val * jnp.exp(-0.5 * z_val * z_val) * (1.0 / math.sqrt(2.0 * math.pi))


def dev(z, y, x):
    return (z * 2 + y) * 4 + x


def send_x(blocks, x_idx):
    own = lax.dynamic_index_in_dim(blocks, x_idx, 0, keepdims=False)
    got = [own]
    for k in (2, 3, 1):
        send = lax.dynamic_index_in_dim(blocks, x_idx ^ k, 0, keepdims=False)
        got.append(lax.ppermute(send, 'dpx', [(i, i ^ k) for i in range(4)]))
    return got


def add_x(got):
    total = got[3].astype(jnp.float32) + got[0].astype(jnp.float32)
    return total + (got[1].astype(jnp.float32) + got[2].astype(jnp.float32))


def shift_z(val, y_rel, zo, yo):
    pairs = [(dev(1 - zo, yo ^ ry, x), dev(zo, yo ^ ry, x)) for ry in y_rel for x in range(4)]
    return lax.ppermute(val, AXES, pairs)


def shift_y(val, z_rel, zo, yo):
    pairs = [(dev(zo ^ rz, 1 - yo, x), dev(zo ^ rz, yo, x)) for rz in z_rel for x in range(4)]
    return lax.ppermute(val, AXES, pairs)


def send_one(part, zo, yo, cut=None):
    half = cut or part.shape[0] // 2
    a_part, b_part = part[:half], part[half:]
    return a_part, b_part, shift_z(a_part, (0, 1), zo, yo), shift_y(b_part, (0, 1), zo, yo)


def add_one(sent):
    return sent[0] + sent[2], sent[1] + sent[3]


def send_two(halves, zo, yo):
    return halves[0], halves[1], shift_y(halves[0], (0,), zo, yo), shift_z(halves[1], (0,), zo, yo)


def after(val, *deps):
    out = lax.optimization_barrier((val,) + deps)
    return out[0], out[1:]


SHARD_ROWS = 4608
N_PIECE = 6
PIECE_ROWS = SHARD_ROWS // N_PIECE
CH_COLS = 512
N_CH = 6
N_PRE = 3
PRE_COLS = N_PRE * CH_COLS
REST_COLS = 3072 - PRE_COLS
X_BIT, Y_BIT, Z_BIT = 1, 2, 4
ADAM_ROWS = 96
C_TOP = 576
ORDERS = ((X_BIT, Y_BIT, Z_BIT), (Y_BIT, Z_BIT, X_BIT), (Z_BIT, X_BIT, Y_BIT)) * 2


def tail_kernel(p_hbm, gd_hbm, qa_hbm, ra_hbm, qb0_hbm, qb1_hbm, rb0_hbm, rb1_hbm, qc0_hbm, qc1_hbm,
                mst_hbm, m_hbm, v_hbm, omst_hbm, om_hbm, ov_hbm, w_hbm,
                own, xrecv, part, a1, b1, a2, b2, sq_a, sq_b, wide_a, wide_b, s_v, mst_v, m_v, v_v, w_v,
                ld_sem, st_sem, c_send, c_recv, xs_send, xs_recv, yz_send, yz_recv, ag_send, ag_recv, dd_send, dd_recv):
    z, y, x = (lax.axis_index(a) for a in AXES)
    ny, nz = 1 - y, 1 - z
    is_late = (z == 1) & (y == 1)
    f32 = jnp.float32

    def x_peer(k):
        if k == 2:
            return lax.rem(x + 2, 4)
        flip = x + 1 - 2 * lax.rem(x, 2)
        return flip if k == 1 else lax.rem(flip + 2, 4)

    peers = {X_BIT: {'dpx': x_peer(2)}, Y_BIT: {'dpy': ny}, Z_BIT: {'dpz': nz}}

    barrier = pltpu.get_barrier_semaphore()
    for where in ({'dpx': x_peer(1)}, {'dpx': x_peer(2)}, {'dpx': x_peer(3)}, {'dpy': ny}, {'dpz': nz}):
        pl.semaphore_signal(barrier, inc=1, device_id=where, device_id_type=pl.DeviceIdType.MESH)
    pl.semaphore_wait(barrier, 5)

    def remote(src, dst, send, recv, where):
        return pltpu.make_async_remote_copy(src_ref=src, dst_ref=dst, send_sem=send, recv_sem=recv,
                                            device_id=where, device_id_type=pl.DeviceIdType.MESH)

    def xs_copy(k, ch):
        lo = (ch - N_PRE) * CH_COLS
        to = x_peer(k)
        return remote(gd_hbm.at[pl.ds(to * 192, 192), pl.ds(lo, CH_COLS)],
                      xrecv.at[k - 1, :, pl.ds(lo, CH_COLS)],
                      xs_send.at[k - 1, ch - N_PRE], xs_recv.at[k - 1, ch - N_PRE], {'dpx': to})

    for ch in range(N_PRE, N_CH):
        for k in (2, 3, 1):
            xs_copy(k, ch).start()

    loads = [pltpu.make_async_copy(p_hbm, part.at[:, pl.ds(0, PRE_COLS)], ld_sem.at[0]),
             pltpu.make_async_copy(gd_hbm.at[pl.ds(x * 192, 192), :], own, ld_sem.at[1]),
             pltpu.make_async_copy(mst_hbm, mst_v, ld_sem.at[2]),
             pltpu.make_async_copy(m_hbm, m_v, ld_sem.at[3]),
             pltpu.make_async_copy(v_hbm, v_v, ld_sem.at[4])]
    for cp in loads:
        cp.start()
    is_a, is_b, is_c = (z == 0) & (y == 0), (z == 0) & (y == 1), (z == 1) & (y == 0)

    def fetch(items):
        return [pltpu.make_async_copy(src, dst, ld_sem.at[5 + i]) for i, (src, dst) in enumerate(items)]

    top_c, bot_c = pl.ds(0, C_TOP), pl.ds(C_TOP, 768 - C_TOP)
    role_loads = {
        'a': (is_a, fetch([(qa_hbm, sq_a), (ra_hbm, sq_b)])),
        'b': (is_b, fetch([(qb0_hbm, wide_a.at[pl.ds(0, 96), :]), (qb1_hbm, wide_a.at[pl.ds(96, 96), :]),
                           (rb0_hbm, wide_b.at[pl.ds(0, 96), :]), (rb1_hbm, wide_b.at[pl.ds(96, 96), :])])),
        'c': (is_c, fetch([(qc0_hbm, sq_a.at[top_c, :]), (qc1_hbm, sq_a.at[bot_c, :])])),
    }
    for role, copies in role_loads.values():
        @pl.when(role)
        def _():
            for cp in copies:
                cp.start()

    def c_copy(kind):
        src, rows, where = ((qc0_hbm, top_c, peers[Y_BIT]), (qc1_hbm, bot_c, peers[Z_BIT]))[kind]
        return remote(src, sq_b.at[rows, :], c_send.at[kind], c_recv.at[kind], where)

    c_sends = (is_late, is_a)

    def spread(terms, groups, tiles):
        def body(g, _):
            rows = pl.ds(pl.multiple_of(g * 8, 8), 8)
            for j in range(tiles):
                cc = pl.ds(128 * j, 128)
                val = terms[0][rows, cc]
                for other in terms[1:]:
                    val = val + other[rows, cc]
                s_v[pl.ds(g * (8 * tiles) + j, 8, stride=tiles), :] = val
            return 0

        lax.fori_loop(0, groups, body, 0)

    loads[0].wait()

    def cols(ch):
        return pl.ds(ch * CH_COLS, CH_COLS)

    top, bot = pl.ds(0, 96), pl.ds(96, 96)

    def yz_copy(kind, ch):
        rows, dst, where = ((top, a1, peers[Z_BIT]), (bot, b1, peers[Y_BIT]),
                            (top, a2, peers[Y_BIT]), (bot, b2, peers[Z_BIT]))[kind]
        return remote(part.at[rows, cols(ch)], dst.at[:, cols(ch)],
                      yz_send.at[kind, ch], yz_recv.at[kind, ch], where)

    yz_sends = {0: z == 0, 1: y == 0, 2: (z == 1) & (y == 0), 3: (z == 0) & (y == 1)}
    yz_takes = {0: z == 1, 1: y == 1, 2: is_late, 3: is_late}

    def yz_start(kind, ch):
        @pl.when(yz_sends[kind])
        def _():
            yz_copy(kind, ch).start()

    def yz_take(kind, ch):
        @pl.when(yz_takes[kind])
        def _():
            yz_copy(kind, ch).wait_recv()
            got = (a1, b1, a2, b2)[kind]
            base = 0 if kind in (0, 2) else 96

            def body(i, _):
                rows = pl.ds(pl.multiple_of(base + i * 8, 8), 8)
                part[rows, cols(ch)] += got[pl.ds(pl.multiple_of(i * 8, 8), 8), cols(ch)]
                return 0

            lax.fori_loop(0, 12, body, 0)

    def x_sum(ch):
        lo = (ch - N_PRE) * CH_COLS
        for k in (2, 3, 1):
            xs_copy(k, ch).wait_recv()

        def body(i, _):
            rows = pl.ds(pl.multiple_of(i * 16, 16), 16)
            cc = pl.ds(lo, CH_COLS)
            part[rows, cols(ch)] = ((own[rows, cc].astype(f32) + xrecv[0, rows, cc].astype(f32))
                                    + (xrecv[1, rows, cc].astype(f32) + xrecv[2, rows, cc].astype(f32)))
            return 0

        lax.fori_loop(0, 12, body, 0)

    def adam():
        def body(i, _):
            rows = pl.ds(pl.multiple_of(i * ADAM_ROWS, ADAM_ROWS), ADAM_ROWS)
            g_sum = s_v[rows, :]
            new_m = BETA_ONE * m_v[rows, :] + (1.0 - BETA_ONE) * g_sum
            new_v = BETA_TWO * v_v[rows, :] + (1.0 - BETA_TWO) * g_sum * g_sum
            m_hat = new_m / (1.0 - BETA_ONE ** STEP)
            v_hat = new_v / (1.0 - BETA_TWO ** STEP)
            new_w = mst_v[rows, :] - LEARN_RATE * m_hat / (jnp.sqrt(v_hat) + ADAM_EPS)
            m_v[rows, :] = new_m
            v_v[rows, :] = new_v
            mst_v[rows, :] = new_w
            w_v[rows, :] = new_w.astype(jnp.bfloat16)
            return 0

        lax.fori_loop(0, SHARD_ROWS // ADAM_ROWS, body, 0)

    def shard_rows(h, r):
        zz = nz if r & Z_BIT else z
        yy = ny if r & Y_BIT else y
        xx = x_peer(2) if r & X_BIT else x
        return pl.ds(pl.multiple_of(((zz * 2 + yy) * 4 + xx) * SHARD_ROWS + h * PIECE_ROWS, 256), PIECE_ROWS)

    def ag_copy(h, r, bit):
        rows = shard_rows(h, r)
        return remote(w_hbm.at[rows, :], w_hbm.at[rows, :], ag_send.at[h, bit.bit_length() - 1, r],
                      ag_recv.at[h, r ^ bit], peers[bit])

    def ag_arrived(h, r):
        rows = shard_rows(h, r)
        bit = ORDERS[h][max(i for i in range(3) if r & ORDERS[h][i])]
        remote(w_hbm.at[rows, :], w_hbm.at[rows, :], ag_send.at[h, 0, r], ag_recv.at[h, r], peers[bit]).wait_recv()

    def dd_copy(h, r):
        rows = shard_rows(h, r)
        return remote(w_hbm.at[rows, :], w_hbm.at[rows, :], dd_send.at[h, r], dd_recv.at[h, r], {'dpx': x_peer(1)})

    def next_bits(h, r):
        last = max([i for i in range(3) if r & ORDERS[h][i]], default=-1)
        return ORDERS[h][last + 1:]

    def hops(step):
        for sub in range(1 << step):
            for h in range(N_PIECE):
                o = ORDERS[h]
                r = o[step] | (o[0] if sub & 1 else 0) | (o[1] if sub & 2 else 0)
                ag_arrived(h, r)
                for bit in next_bits(h, r):
                    ag_copy(h, r, bit).start()
                dd_copy(h, r).start()

    outs = [pltpu.make_async_copy(mst_v, omst_hbm, st_sem.at[0]),
            pltpu.make_async_copy(m_v, om_hbm, st_sem.at[1]),
            pltpu.make_async_copy(v_v, ov_hbm, st_sem.at[2])]

    def own_update():
        adam()
        mine = shard_rows(0, 0)
        rows = pl.ds(mine.start, SHARD_ROWS)
        put = pltpu.make_async_copy(w_v, w_hbm.at[rows, :], st_sem.at[3])
        put.start()
        for cp in outs:
            cp.start()
        put.wait()

    for ch in range(N_PRE):
        yz_start(0, ch)
        yz_start(1, ch)
    for cp in loads[1:]:
        cp.wait()

    @pl.when(is_late)
    def _():
        c_copy(0).start()

    for name, terms, groups, tiles in (('a', (sq_a, sq_b), 96, 6), ('b', (wide_a, wide_b), 24, 24)):
        role, copies = role_loads[name]

        @pl.when(role)
        def _():
            for cp in copies:
                cp.wait()
            spread(terms, groups, tiles)
            own_update()

    for ch in range(N_PRE):
        yz_take(0, ch)
        yz_take(1, ch)
        yz_start(2, ch)
        yz_start(3, ch)
    for ch in range(N_PRE, N_CH):
        x_sum(ch)
        yz_start(0, ch)
        yz_start(1, ch)
        if ch == N_PRE:
            @pl.when(is_a)
            def _():
                c_copy(1).start()
    for ch in range(N_PRE, N_CH):
        yz_take(0, ch)
        yz_take(1, ch)
        yz_start(2, ch)
        yz_start(3, ch)

    @pl.when(is_late)
    def _():
        for ch in range(N_CH):
            for kind in (2, 3):
                yz_take(kind, ch)

        spread((part,), 24, 24)
        own_update()

    @pl.when(is_c)
    def _():
        for cp in role_loads['c'][1]:
            cp.wait()
        for kind in (0, 1):
            c_copy(kind).wait_recv()
        spread((sq_a, sq_b), 96, 6)
        own_update()

    for step in range(3):
        for h in range(N_PIECE):
            ag_copy(h, 0, ORDERS[h][step]).start()
    for h in range(N_PIECE):
        dd_copy(h, 0).start()
    for step in range(3):
        hops(step)

    for h in range(N_PIECE):
        for r in range(8):
            for bit in next_bits(h, r):
                ag_copy(h, r, bit).wait_send()
            dd_copy(h, r).wait()
    for ch in range(N_PRE, N_CH):
        for k in (1, 2, 3):
            xs_copy(k, ch).wait_send()
    for ch in range(N_CH):
        for kind in range(4):
            @pl.when(yz_sends[kind])
            def _():
                yz_copy(kind, ch).wait_send()
    for kind in (0, 1):
        @pl.when(c_sends[kind])
        def _():
            c_copy(kind).wait_send()
    for cp in outs:
        cp.wait()


def tail(*args):
    any_spec = pl.BlockSpec(memory_space=pl.ANY)
    f32, bf16 = jnp.float32, jnp.bfloat16
    dma = pltpu.SemaphoreType.DMA
    shard = pltpu.VMEM((SHARD_ROWS, 128), f32)
    half = pltpu.VMEM((96, 3072), f32)
    return pl.pallas_call(
        tail_kernel,
        out_shape=(shard, shard, shard, pltpu.VMEM((16 * SHARD_ROWS, 128), bf16)),
        in_specs=[any_spec] * 13,
        out_specs=[any_spec] * 4,
        scratch_shapes=[
            pltpu.VMEM((192, REST_COLS), bf16), pltpu.VMEM((3, 192, REST_COLS), bf16), pltpu.VMEM((192, 3072), f32),
            half, half, half, half, pltpu.VMEM((768, 768), f32), pltpu.VMEM((768, 768), f32),
            pltpu.VMEM((192, 3072), f32), pltpu.VMEM((192, 3072), f32),
            shard, shard, shard, shard, pltpu.VMEM((SHARD_ROWS, 128), bf16),
            dma((9,)), dma((4,)), dma((2,)), dma((2,)),
            dma((3, N_CH - N_PRE)), dma((3, N_CH - N_PRE)), dma((4, N_CH)), dma((4, N_CH)),
            dma((N_PIECE, 3, 8)), dma((N_PIECE, 8)), dma((N_PIECE, 8)), dma((N_PIECE, 8)),
        ],
        compiler_params=pltpu.CompilerParams(collective_id=0, has_side_effects=True, vmem_limit_bytes=31 << 20),
        name="tail",
    )(*args)


def solution(mesh):
    def inner_step(x_one, dy_one, w1_in, w1_out, w2_in, w2_out, master, adam_m, adam_v):
        xi = lax.axis_index('dpx')
        f32, bf16 = jnp.float32, jnp.bfloat16

        def mm(spec, a, b):
            return jnp.einsum(spec, a, b, preferred_element_type=f32)

        z_one = mm('td,df->tf', x_one, w1_in).astype(bf16)
        h_one = gelu_value(z_one.astype(f32)).astype(bf16)
        z_one, h_one = lax.optimization_barrier((z_one, h_one))
        x_two = (x_one.astype(f32) + mm('tf,fd->td', h_one, w1_out)).astype(bf16)
        z_two = mm('td,df->tf', x_two, w2_in).astype(bf16)
        h_two = gelu_value(z_two.astype(f32)).astype(bf16)
        z_two, h_two = lax.optimization_barrier((z_two, h_two))
        g_a = mm('tf,td->fd', h_two, dy_one).astype(bf16)
        x_a = send_x(g_a.reshape(4, 768, 768), xi)
        dz_two = (mm('td,fd->tf', dy_one, w2_out) * gelu_slope(z_two.astype(f32))).astype(bf16)
        g_b = mm('td,tf->df', x_two, dz_two).astype(bf16)
        x_b = send_x(g_b.reshape(4, 192, 3072), xi)
        p_a = add_x(x_a)
        dz_two, (p_a,) = after(dz_two, p_a)
        one_a = shift_z(p_a, (0, 1), 0, 0)
        dx_two = (dy_one.astype(f32) + mm('tf,df->td', dz_two, w2_in)).astype(bf16)
        g_c = mm('tf,td->fd', h_one, dx_two).astype(bf16)
        x_c = send_x(g_c.reshape(4, 768, 768), xi)
        p_b = add_x(x_b)
        dx_two, (p_b, q_a) = after(dx_two, p_b, p_a + one_a)
        two_a = shift_y(q_a, (0,), 0, 0)
        one_b = send_one(p_b, 0, 1)
        dz_one = (mm('td,fd->tf', dx_two, w1_out) * gelu_slope(z_one.astype(f32))).astype(bf16)
        p_c = add_x(x_c)
        dz_one, (qb0, qb1, p_c) = after(dz_one, *add_one(one_b), p_c)
        two_b = send_two((qb0, qb1), 0, 1)
        one_c = send_one(p_c, 1, 0, C_TOP)
        g_d0 = mm('td,tf->df', x_one, dz_one[:, :PRE_COLS]).astype(bf16)
        x_d0 = send_x(g_d0.reshape(4, 192, PRE_COLS), xi)
        g_d1 = mm('td,tf->df', x_one, dz_one[:, PRE_COLS:]).astype(bf16)
        qc0, qc1 = add_one(one_c)
        flat = lambda t: t.reshape(SHARD_ROWS, 128)
        new_master, new_m, new_v, weights = tail(
            add_x(x_d0), g_d1, q_a, two_a, qb0, qb1, two_b[2], two_b[3], qc0, qc1,
            flat(master), flat(adam_m), flat(adam_v))
        return new_master.reshape(-1), new_m.reshape(-1), new_v.reshape(-1), weights.reshape(-1)

    in_specs = (P(AXES, None), P(AXES, None), P(), P(), P(), P(), P(AXES), P(AXES), P(AXES))
    out_specs = (P(AXES), P(AXES), P(AXES), P())
    return jax.shard_map(inner_step, mesh=mesh, in_specs=in_specs, out_specs=out_specs, check_vma=False)
```

```python
import math
import jax
import jax.numpy as jnp
from jax import lax
from jax.experimental import pallas as pl
from jax.experimental.pallas import tpu as pltpu
from jax.sharding import PartitionSpec as P

AXES = ('dpz', 'dpy', 'dpx')
STEP = 10
BETA_ONE = 0.9
BETA_TWO = 0.999
LEARN_RATE = 0.001
ADAM_EPS = 1e-8


def gelu_value(z_val):
    return 0.5 * z_val * (1.0 + lax.erf(z_val * (1.0 / math.sqrt(2.0))))


def gelu_slope(z_val):
    cdf_part = 0.5 * (1.0 + lax.erf(z_val * (1.0 / math.sqrt(2.0))))
    return cdf_part + z_val * jnp.exp(-0.5 * z_val * z_val) * (1.0 / math.sqrt(2.0 * math.pi))


def dev(z, y, x):
    return (z * 2 + y) * 4 + x


def send_x(blocks, x_idx):
    got = []
    for k in (2, 3, 1):
        send = lax.dynamic_index_in_dim(blocks, x_idx ^ k, 0, keepdims=False)
        got.append(lax.ppermute(send, 'dpx', [(i, i ^ k) for i in range(4)]))
    return got


def add_x(blocks, x_idx, got):
    own = lax.dynamic_index_in_dim(blocks, x_idx, 0, keepdims=False)
    total = got[2].astype(jnp.float32) + own.astype(jnp.float32)
    return total + (got[0].astype(jnp.float32) + got[1].astype(jnp.float32))


def shift_z(val, y_rel, zo, yo):
    pairs = [(dev(1 - zo, yo ^ ry, x), dev(zo, yo ^ ry, x)) for ry in y_rel for x in range(4)]
    return lax.ppermute(val, AXES, pairs)


def shift_y(val, z_rel, zo, yo):
    pairs = [(dev(zo ^ rz, 1 - yo, x), dev(zo ^ rz, yo, x)) for rz in z_rel for x in range(4)]
    return lax.ppermute(val, AXES, pairs)


def send_one(part, zo, yo, cut=None):
    half = cut or part.shape[0] // 2
    a_part, b_part = part[:half], part[half:]
    return a_part, b_part, shift_z(a_part, (0, 1), zo, yo), shift_y(b_part, (0, 1), zo, yo)


def add_one(sent):
    return sent[0] + sent[2], sent[1] + sent[3]


def send_two(halves, zo, yo):
    return halves[0], halves[1], shift_y(halves[0], (0,), zo, yo), shift_z(halves[1], (0,), zo, yo)


def after(val, *deps):
    out = lax.optimization_barrier((val,) + deps)
    return out[0], out[1:]


SHARD_ROWS = 4608
N_PIECE = 6
PIECE_ROWS = SHARD_ROWS // N_PIECE
CH_COLS = 512
N_CH = 6
N_PRE = 4
PIECE_COLS = 1024
X_BIT, Y_BIT, Z_BIT = 1, 2, 4
ADAM_ROWS = 96
C_TOP = 480
ORDERS = ((X_BIT, Y_BIT, Z_BIT), (Y_BIT, Z_BIT, X_BIT), (Z_BIT, X_BIT, Y_BIT)) * 2


def tail_kernel(gd0_hbm, gd1_hbm, gd_hbm, d0k2, d0k3, d0k1, d1k2, d1k3, d1k1,
                qa_hbm, ra_hbm, qb0_hbm, qb1_hbm, rb0_hbm, rb1_hbm, pc0_hbm, pc1_hbm, rc0_hbm, rc1_hbm,
                mst_hbm, m_hbm, v_hbm, omst_hbm, om_hbm, ov_hbm, w_hbm,
                own, xrecv, part, a1, b1, a2, b2, sq_a, sq_b, c_a, c_b, wide_a, wide_b, s_v, mst_v, m_v, v_v, w_v,
                ld_sem, st_sem, c_send, c_recv, xs_send, xs_recv, yz_send, yz_recv, ag_send, ag_recv, dd_send, dd_recv):
    z, y, x = (lax.axis_index(a) for a in AXES)
    ny, nz = 1 - y, 1 - z
    is_late = (z == 1) & (y == 1)
    f32 = jnp.float32

    def x_peer(k):
        if k == 2:
            return lax.rem(x + 2, 4)
        flip = x + 1 - 2 * lax.rem(x, 2)
        return flip if k == 1 else lax.rem(flip + 2, 4)

    peers = {X_BIT: {'dpx': x_peer(2)}, Y_BIT: {'dpy': ny}, Z_BIT: {'dpz': nz}}

    barrier = pltpu.get_barrier_semaphore()
    for where in ({'dpx': x_peer(1)}, {'dpx': x_peer(2)}, {'dpx': x_peer(3)}, {'dpy': ny}, {'dpz': nz}):
        pl.semaphore_signal(barrier, inc=1, device_id=where, device_id_type=pl.DeviceIdType.MESH)
    pl.semaphore_wait(barrier, 5)

    def remote(src, dst, send, recv, where):
        return pltpu.make_async_remote_copy(src_ref=src, dst_ref=dst, send_sem=send, recv_sem=recv,
                                            device_id=where, device_id_type=pl.DeviceIdType.MESH)

    def cols(ch):
        return pl.ds(ch * CH_COLS, CH_COLS)

    def xs_copy(k, ch):
        lo = (ch - N_PRE) * CH_COLS
        to = x_peer(k)
        return remote(gd_hbm.at[pl.ds(to * 192, 192), pl.ds(lo, CH_COLS)],
                      xrecv.at[k - 1, :, cols(ch)],
                      xs_send.at[k - 1, ch - N_PRE], xs_recv.at[k - 1, ch - N_PRE], {'dpx': to})

    for ch in range(N_PRE, N_CH):
        for k in (2, 3, 1):
            xs_copy(k, ch).start()

    mine = pl.ds(x * 192, 192)
    pre = []
    for part_no, (grad, got) in enumerate(((gd0_hbm, (d0k1, d0k2, d0k3)), (gd1_hbm, (d1k1, d1k2, d1k3)))):
        cc = pl.ds(part_no * PIECE_COLS, PIECE_COLS)
        pre.append((grad.at[mine, :], own.at[:, cc]))
        pre.extend((got[k], xrecv.at[k, :, cc]) for k in range(3))
    state = [(gd_hbm.at[mine, :], own.at[:, pl.ds(2 * PIECE_COLS, PIECE_COLS)]),
             (mst_hbm, mst_v), (m_hbm, m_v), (v_hbm, v_v)]
    loads = [pltpu.make_async_copy(src, dst, ld_sem.at[i]) for i, (src, dst) in enumerate(pre + state)]
    for cp in loads:
        cp.start()
    is_a, is_b, is_c = (z == 0) & (y == 0), (z == 0) & (y == 1), (z == 1) & (y == 0)

    def fetch(items, base=12):
        return [pltpu.make_async_copy(src, dst, ld_sem.at[base + i]) for i, (src, dst) in enumerate(items)]

    top_c, bot_c = pl.ds(0, C_TOP), pl.ds(C_TOP, 768 - C_TOP)
    role_loads = {
        'a': (is_a, fetch([(qa_hbm, sq_a), (ra_hbm, sq_b)])),
        'b': (is_b, fetch([(qb0_hbm, wide_a.at[pl.ds(0, 96), :]), (qb1_hbm, wide_a.at[pl.ds(96, 96), :]),
                           (rb0_hbm, wide_b.at[pl.ds(0, 96), :]), (rb1_hbm, wide_b.at[pl.ds(96, 96), :])])),
        'c': (is_c, fetch([(pc0_hbm, c_a.at[top_c, :]), (pc1_hbm, c_a.at[bot_c, :]),
                           (rc0_hbm, c_b.at[top_c, :]), (rc1_hbm, c_b.at[bot_c, :])])),
        'send0': (is_late, fetch([(pc0_hbm, c_a.at[top_c, :]), (rc0_hbm, c_b.at[top_c, :])], 16)),
        'send1': (is_a, fetch([(pc1_hbm, c_a.at[bot_c, :]), (rc1_hbm, c_b.at[bot_c, :])], 16)),
    }
    for role, copies in role_loads.values():
        @pl.when(role)
        def _():
            for cp in copies:
                cp.start()

    def c_copy(kind):
        rows, where = ((top_c, peers[Y_BIT]), (bot_c, peers[Z_BIT]))[kind]
        return remote(c_a.at[rows, :], sq_b.at[rows, :], c_send.at[kind], c_recv.at[kind], where)

    c_sends = (is_late, is_a)

    def c_add(kind):
        for cp in role_loads['send%d' % kind][1]:
            cp.wait()
        lo, count = ((0, C_TOP), (C_TOP, 768 - C_TOP))[kind]

        def body(i, _):
            rows = pl.ds(pl.multiple_of(lo + i * 16, 16), 16)
            c_a[rows, :] += c_b[rows, :]
            return 0

        lax.fori_loop(0, count // 16, body, 0)

    def spread(terms, groups, tiles):
        def body(g, _):
            rows = pl.ds(pl.multiple_of(g * 8, 8), 8)
            for j in range(tiles):
                cc = pl.ds(128 * j, 128)
                val = terms[0][rows, cc]
                for other in terms[1:]:
                    val = val + other[rows, cc]
                s_v[pl.ds(g * (8 * tiles) + j, 8, stride=tiles), :] = val
            return 0

        lax.fori_loop(0, groups, body, 0)

    for cp in loads[:len(pre)]:
        cp.wait()

    top, bot = pl.ds(0, 96), pl.ds(96, 96)

    def yz_copy(kind, ch):
        rows, dst, where = ((top, a1, peers[Z_BIT]), (bot, b1, peers[Y_BIT]),
                            (top, a2, peers[Y_BIT]), (bot, b2, peers[Z_BIT]))[kind]
        return remote(part.at[rows, cols(ch)], dst.at[:, cols(ch)],
                      yz_send.at[kind, ch], yz_recv.at[kind, ch], where)

    yz_sends = {0: z == 0, 1: y == 0, 2: (z == 1) & (y == 0), 3: (z == 0) & (y == 1)}
    yz_takes = {0: z == 1, 1: y == 1, 2: is_late, 3: is_late}

    def yz_start(kind, ch):
        @pl.when(yz_sends[kind])
        def _():
            yz_copy(kind, ch).start()

    def yz_take(kind, ch):
        @pl.when(yz_takes[kind])
        def _():
            yz_copy(kind, ch).wait_recv()
            got = (a1, b1, a2, b2)[kind]
            base = 0 if kind in (0, 2) else 96

            def body(i, _):
                rows = pl.ds(pl.multiple_of(base + i * 8, 8), 8)
                part[rows, cols(ch)] += got[pl.ds(pl.multiple_of(i * 8, 8), 8), cols(ch)]
                return 0

            lax.fori_loop(0, 12, body, 0)

    def x_sum(ch):
        if ch >= N_PRE:
            for k in (2, 3, 1):
                xs_copy(k, ch).wait_recv()

        def body(i, _):
            rows = pl.ds(pl.multiple_of(i * 16, 16), 16)
            part[rows, cols(ch)] = ((own[rows, cols(ch)].astype(f32) + xrecv[0, rows, cols(ch)].astype(f32))
                                    + (xrecv[1, rows, cols(ch)].astype(f32) + xrecv[2, rows, cols(ch)].astype(f32)))
            return 0

        lax.fori_loop(0, 12, body, 0)

    def adam():
        def body(i, _):
            rows = pl.ds(pl.multiple_of(i * ADAM_ROWS, ADAM_ROWS), ADAM_ROWS)
            g_sum = s_v[rows, :]
            new_m = BETA_ONE * m_v[rows, :] + (1.0 - BETA_ONE) * g_sum
            new_v = BETA_TWO * v_v[rows, :] + (1.0 - BETA_TWO) * g_sum * g_sum
            m_hat = new_m / (1.0 - BETA_ONE ** STEP)
            v_hat = new_v / (1.0 - BETA_TWO ** STEP)
            new_w = mst_v[rows, :] - LEARN_RATE * m_hat / (jnp.sqrt(v_hat) + ADAM_EPS)
            m_v[rows, :] = new_m
            v_v[rows, :] = new_v
            mst_v[rows, :] = new_w
            w_v[rows, :] = new_w.astype(jnp.bfloat16)
            return 0

        lax.fori_loop(0, SHARD_ROWS // ADAM_ROWS, body, 0)

    def shard_rows(h, r):
        zz = nz if r & Z_BIT else z
        yy = ny if r & Y_BIT else y
        xx = x_peer(2) if r & X_BIT else x
        return pl.ds(pl.multiple_of(((zz * 2 + yy) * 4 + xx) * SHARD_ROWS + h * PIECE_ROWS, 256), PIECE_ROWS)

    def ag_copy(h, r, bit):
        rows = shard_rows(h, r)
        return remote(w_hbm.at[rows, :], w_hbm.at[rows, :], ag_send.at[h, bit.bit_length() - 1, r],
                      ag_recv.at[h, r ^ bit], peers[bit])

    def ag_arrived(h, r):
        rows = shard_rows(h, r)
        bit = ORDERS[h][max(i for i in range(3) if r & ORDERS[h][i])]
        remote(w_hbm.at[rows, :], w_hbm.at[rows, :], ag_send.at[h, 0, r], ag_recv.at[h, r], peers[bit]).wait_recv()

    def dd_copy(h, r):
        rows = shard_rows(h, r)
        return remote(w_hbm.at[rows, :], w_hbm.at[rows, :], dd_send.at[h, r], dd_recv.at[h, r], {'dpx': x_peer(1)})

    def next_bits(h, r):
        last = max([i for i in range(3) if r & ORDERS[h][i]], default=-1)
        return ORDERS[h][last + 1:]

    def hops(step):
        for sub in range(1 << step):
            for h in range(N_PIECE):
                o = ORDERS[h]
                r = o[step] | (o[0] if sub & 1 else 0) | (o[1] if sub & 2 else 0)
                ag_arrived(h, r)
                for bit in next_bits(h, r):
                    ag_copy(h, r, bit).start()
                dd_copy(h, r).start()

    outs = [pltpu.make_async_copy(mst_v, omst_hbm, st_sem.at[0]),
            pltpu.make_async_copy(m_v, om_hbm, st_sem.at[1]),
            pltpu.make_async_copy(v_v, ov_hbm, st_sem.at[2])]

    def own_update():
        adam()
        mine = shard_rows(0, 0)
        rows = pl.ds(mine.start, SHARD_ROWS)
        put = pltpu.make_async_copy(w_v, w_hbm.at[rows, :], st_sem.at[3])
        put.start()
        for cp in outs:
            cp.start()
        put.wait()

    for ch in range(N_PRE):
        x_sum(ch)
        yz_start(0, ch)
        yz_start(1, ch)
    for cp in loads[len(pre):]:
        cp.wait()

    @pl.when(is_late)
    def _():
        c_add(0)
        c_copy(0).start()

    @pl.when(is_a)
    def _():
        c_add(1)

    for name, terms, groups, tiles in (('a', (sq_a, sq_b), 96, 6), ('b', (wide_a, wide_b), 24, 24)):
        role, copies = role_loads[name]

        @pl.when(role)
        def _():
            for cp in copies:
                cp.wait()
            spread(terms, groups, tiles)
            own_update()

    for ch in range(N_PRE):
        yz_take(0, ch)
        yz_take(1, ch)
        yz_start(2, ch)
        yz_start(3, ch)
    for ch in range(N_PRE, N_CH):
        x_sum(ch)
        yz_start(0, ch)
        yz_start(1, ch)
        if ch == N_PRE:
            @pl.when(is_a)
            def _():
                c_copy(1).start()
    for ch in range(N_PRE, N_CH):
        yz_take(0, ch)
        yz_take(1, ch)
        yz_start(2, ch)
        yz_start(3, ch)

    @pl.when(is_late)
    def _():
        for ch in range(N_CH):
            for kind in (2, 3):
                yz_take(kind, ch)

        spread((part,), 24, 24)
        own_update()

    @pl.when(is_c)
    def _():
        for cp in role_loads['c'][1]:
            cp.wait()
        for kind in (0, 1):
            c_copy(kind).wait_recv()
        spread((c_a, c_b, sq_b), 96, 6)
        own_update()

    for step in range(3):
        for h in range(N_PIECE):
            ag_copy(h, 0, ORDERS[h][step]).start()
    for h in range(N_PIECE):
        dd_copy(h, 0).start()
    for step in range(3):
        hops(step)

    for h in range(N_PIECE):
        for r in range(8):
            for bit in next_bits(h, r):
                ag_copy(h, r, bit).wait_send()
            dd_copy(h, r).wait()
    for ch in range(N_PRE, N_CH):
        for k in (1, 2, 3):
            xs_copy(k, ch).wait_send()
    for ch in range(N_CH):
        for kind in range(4):
            @pl.when(yz_sends[kind])
            def _():
                yz_copy(kind, ch).wait_send()
    for kind in (0, 1):
        @pl.when(c_sends[kind])
        def _():
            c_copy(kind).wait_send()
    for cp in outs:
        cp.wait()


def tail(*args):
    any_spec = pl.BlockSpec(memory_space=pl.ANY)
    f32, bf16 = jnp.float32, jnp.bfloat16
    dma = pltpu.SemaphoreType.DMA
    shard = pltpu.VMEM((SHARD_ROWS, 128), f32)
    half = pltpu.VMEM((96, 3072), f32)
    square = pltpu.VMEM((768, 768), f32)
    return pl.pallas_call(
        tail_kernel,
        out_shape=(shard, shard, shard, pltpu.VMEM((16 * SHARD_ROWS, 128), bf16)),
        in_specs=[any_spec] * len(args),
        out_specs=[any_spec] * 4,
        scratch_shapes=[
            pltpu.VMEM((192, 3072), bf16), pltpu.VMEM((3, 192, 3072), bf16), pltpu.VMEM((192, 3072), f32),
            half, half, half, half, square, square, square, square,
            pltpu.VMEM((192, 3072), f32), pltpu.VMEM((192, 3072), f32),
            shard, shard, shard, shard, pltpu.VMEM((SHARD_ROWS, 128), bf16),
            dma((18,)), dma((4,)), dma((2,)), dma((2,)),
            dma((3, N_CH - N_PRE)), dma((3, N_CH - N_PRE)), dma((4, N_CH)), dma((4, N_CH)),
            dma((N_PIECE, 3, 8)), dma((N_PIECE, 8)), dma((N_PIECE, 8)), dma((N_PIECE, 8)),
        ],
        compiler_params=pltpu.CompilerParams(collective_id=0, has_side_effects=True, vmem_limit_bytes=38 << 20),
        name="tail",
    )(*args)


def slope_product(grad, weight, pre):
    rows, cols, sub = 1024, 1536, 256

    def kernel(grad_ref, weight_ref, pre_ref, out_ref):
        for i in range(rows // sub):
            part = pl.ds(i * sub, sub)
            up = lax.dot_general(grad_ref[part, :], weight_ref[...], (((1,), (1,)), ((), ())),
                                 preferred_element_type=jnp.float32)
            out_ref[part, :] = (up * gelu_slope(pre_ref[part, :].astype(jnp.float32))).astype(jnp.bfloat16)

    tokens, width = grad.shape
    full = weight.shape[0]
    return pl.pallas_call(
        kernel,
        grid=(full // cols, tokens // rows),
        in_specs=[pl.BlockSpec((rows, width), lambda j, i: (i, 0)),
                  pl.BlockSpec((cols, width), lambda j, i: (j, 0)),
                  pl.BlockSpec((rows, cols), lambda j, i: (i, j))],
        out_specs=pl.BlockSpec((rows, cols), lambda j, i: (i, j)),
        out_shape=jax.ShapeDtypeStruct((tokens, full), jnp.bfloat16),
        compiler_params=pltpu.CompilerParams(vmem_limit_bytes=40 << 20),
        cost_estimate=pl.CostEstimate(flops=2 * tokens * width * full, bytes_accessed=4 * tokens * full,
                                      transcendentals=tokens * full),
        name="slope_product",
    )(grad, weight, pre)


def solution(mesh):
    def inner_step(x_one, dy_one, w1_in, w1_out, w2_in, w2_out, master, adam_m, adam_v):
        xi = lax.axis_index('dpx')
        f32, bf16 = jnp.float32, jnp.bfloat16

        def mm(spec, a, b):
            return jnp.einsum(spec, a, b, preferred_element_type=f32)

        z_one = mm('td,df->tf', x_one, w1_in).astype(bf16)
        h_one = gelu_value(z_one.astype(f32)).astype(bf16)
        z_one, h_one = lax.optimization_barrier((z_one, h_one))
        x_two = (x_one.astype(f32) + mm('tf,fd->td', h_one, w1_out)).astype(bf16)
        z_two = mm('td,df->tf', x_two, w2_in).astype(bf16)
        h_two = gelu_value(z_two.astype(f32)).astype(bf16)
        z_two, h_two = lax.optimization_barrier((z_two, h_two))
        g_a = mm('tf,td->fd', h_two, dy_one).astype(bf16)
        x_a = send_x(g_a.reshape(4, 768, 768), xi)
        dz_two = slope_product(dy_one, w2_out, z_two)
        g_b = mm('td,tf->df', x_two, dz_two).astype(bf16)
        x_b = send_x(g_b.reshape(4, 192, 3072), xi)
        p_a = add_x(g_a.reshape(4, 768, 768), xi, x_a)
        dz_two, (p_a,) = after(dz_two, p_a)
        one_a = shift_z(p_a, (0, 1), 0, 0)
        dx_two = (dy_one.astype(f32) + mm('tf,df->td', dz_two, w2_in)).astype(bf16)
        g_c = mm('tf,td->fd', h_one, dx_two).astype(bf16)
        x_c = send_x(g_c.reshape(4, 768, 768), xi)
        p_b = add_x(g_b.reshape(4, 192, 3072), xi, x_b)
        dx_two, (p_b, q_a) = after(dx_two, p_b, p_a + one_a)
        two_a = shift_y(q_a, (0,), 0, 0)
        one_b = send_one(p_b, 0, 1)
        dz_one = slope_product(dx_two, w1_out, z_one)
        dz_one, (qb0, qb1) = after(dz_one, *add_one(one_b))
        two_b = send_two((qb0, qb1), 0, 1)

        def last_piece(grad, i):
            return mm('td,tf->df', x_one, grad[:, i * PIECE_COLS:(i + 1) * PIECE_COLS]).astype(bf16)

        g_d0 = last_piece(dz_one, 0)
        x_d0 = send_x(g_d0.reshape(4, 192, PIECE_COLS), xi)
        p_c = add_x(g_c.reshape(4, 768, 768), xi, x_c)
        dz_one, (p_c,) = after(dz_one, p_c)
        one_c = send_one(p_c, 1, 0, C_TOP)
        g_d1 = last_piece(dz_one, 1)
        x_d1 = send_x(g_d1.reshape(4, 192, PIECE_COLS), xi)
        g_d2 = last_piece(dz_one, 2)
        flat = lambda t: t.reshape(SHARD_ROWS, 128)
        new_master, new_m, new_v, weights = tail(
            g_d0, g_d1, g_d2, *x_d0, *x_d1, q_a, two_a, qb0, qb1, two_b[2], two_b[3], *one_c,
            flat(master), flat(adam_m), flat(adam_v))
        return new_master.reshape(-1), new_m.reshape(-1), new_v.reshape(-1), weights.reshape(-1)

    in_specs = (P(AXES, None), P(AXES, None), P(), P(), P(), P(), P(AXES), P(AXES), P(AXES))
    out_specs = (P(AXES), P(AXES), P(AXES), P())
    return jax.shard_map(inner_step, mesh=mesh, in_specs=in_specs, out_specs=out_specs, check_vma=False)
```

```python
import math
import jax
import jax.numpy as jnp
from jax import lax
from jax.experimental import pallas as pl
from jax.experimental.pallas import tpu as pltpu
from jax.sharding import PartitionSpec as P

AXES = ('dpz', 'dpy', 'dpx')
STEP = 10
BETA_ONE = 0.9
BETA_TWO = 0.999
LEARN_RATE = 0.001
ADAM_EPS = 1e-8


def gelu_value(z_val):
    return 0.5 * z_val * (1.0 + lax.erf(z_val * (1.0 / math.sqrt(2.0))))


def gelu_slope(z_val):
    cdf_part = 0.5 * (1.0 + lax.erf(z_val * (1.0 / math.sqrt(2.0))))
    return cdf_part + z_val * jnp.exp(-0.5 * z_val * z_val) * (1.0 / math.sqrt(2.0 * math.pi))


def dev(z, y, x):
    return (z * 2 + y) * 4 + x


def send_x(blocks, x_idx):
    got = []
    for k in (2, 3, 1):
        send = lax.dynamic_index_in_dim(blocks, x_idx ^ k, 0, keepdims=False)
        got.append(lax.ppermute(send, 'dpx', [(i, i ^ k) for i in range(4)]))
    return got


def add_x(blocks, x_idx, got):
    own = lax.dynamic_index_in_dim(blocks, x_idx, 0, keepdims=False)
    total = got[2].astype(jnp.float32) + own.astype(jnp.float32)
    return total + (got[0].astype(jnp.float32) + got[1].astype(jnp.float32))


def shift_z(val, y_rel, zo, yo):
    pairs = [(dev(1 - zo, yo ^ ry, x), dev(zo, yo ^ ry, x)) for ry in y_rel for x in range(4)]
    return lax.ppermute(val, AXES, pairs)


def shift_y(val, z_rel, zo, yo):
    pairs = [(dev(zo ^ rz, 1 - yo, x), dev(zo ^ rz, yo, x)) for rz in z_rel for x in range(4)]
    return lax.ppermute(val, AXES, pairs)


def send_one(part, zo, yo, cut=None):
    half = cut or part.shape[0] // 2
    a_part, b_part = part[:half], part[half:]
    return a_part, b_part, shift_z(a_part, (0, 1), zo, yo), shift_y(b_part, (0, 1), zo, yo)


def add_one(sent):
    return sent[0] + sent[2], sent[1] + sent[3]


def send_two(halves, zo, yo):
    return halves[0], halves[1], shift_y(halves[0], (0,), zo, yo), shift_z(halves[1], (0,), zo, yo)


def after(val, *deps):
    out = lax.optimization_barrier((val,) + deps)
    return out[0], out[1:]


SHARD_ROWS = 4608
N_PIECE = 6
PIECE_ROWS = SHARD_ROWS // N_PIECE
CH_COLS = 256
N_CH = 12
N_PRE = 8
PIECE_COLS = 1024
X_BIT, Y_BIT, Z_BIT = 1, 2, 4
ADAM_ROWS = 96
C_TOP = 528
D_TOP = 80
ORDERS = ((X_BIT, Y_BIT, Z_BIT), (Y_BIT, Z_BIT, X_BIT), (Z_BIT, X_BIT, Y_BIT)) * 2


def tail_kernel(gd0_hbm, gd1_hbm, gd_hbm, d0k2, d0k3, d0k1, d1k2, d1k3, d1k1,
                qa_hbm, ra_hbm, qb0_hbm, qb1_hbm, rb0_hbm, rb1_hbm, pc0_hbm, pc1_hbm, rc0_hbm, rc1_hbm,
                mst_hbm, m_hbm, v_hbm, omst_hbm, om_hbm, ov_hbm, w_hbm,
                own, xrecv, part, top_got, bot_got, sq_a, sq_b, c_a, c_b, wide_a, wide_b, s_v, mst_v, m_v, v_v, w_v,
                ld_sem, st_sem, c_send, c_recv, xs_send, xs_recv, yz_send, yz_recv, ag_send, ag_recv, dd_send, dd_recv):
    z, y, x = (lax.axis_index(a) for a in AXES)
    ny, nz = 1 - y, 1 - z
    is_late = (z == 1) & (y == 1)
    is_a, is_b, is_c = (z == 0) & (y == 0), (z == 0) & (y == 1), (z == 1) & (y == 0)
    f32 = jnp.float32

    def x_peer(k):
        if k == 2:
            return lax.rem(x + 2, 4)
        flip = x + 1 - 2 * lax.rem(x, 2)
        return flip if k == 1 else lax.rem(flip + 2, 4)

    peers = {X_BIT: {'dpx': x_peer(2)}, Y_BIT: {'dpy': ny}, Z_BIT: {'dpz': nz}}

    barrier = pltpu.get_barrier_semaphore()
    for where in ({'dpx': x_peer(1)}, {'dpx': x_peer(2)}, {'dpx': x_peer(3)}, {'dpy': ny}, {'dpz': nz}):
        pl.semaphore_signal(barrier, inc=1, device_id=where, device_id_type=pl.DeviceIdType.MESH)
    pl.semaphore_wait(barrier, 5)

    def remote(src, dst, send, recv, where):
        return pltpu.make_async_remote_copy(src_ref=src, dst_ref=dst, send_sem=send, recv_sem=recv,
                                            device_id=where, device_id_type=pl.DeviceIdType.MESH)

    def cols(ch):
        return pl.ds(ch * CH_COLS, CH_COLS)

    def xs_copy(k, ch):
        lo = (ch - N_PRE) * CH_COLS
        to = x_peer(k)
        return remote(gd_hbm.at[pl.ds(to * 192, 192), pl.ds(lo, CH_COLS)],
                      xrecv.at[k - 1, :, cols(ch)],
                      xs_send.at[k - 1, ch - N_PRE], xs_recv.at[k - 1, ch - N_PRE], {'dpx': to})

    for ch in range(N_PRE, N_CH):
        for k in (2, 3, 1):
            xs_copy(k, ch).start()

    mine = pl.ds(x * 192, 192)
    pre = []
    for part_no, (grad, got) in enumerate(((gd0_hbm, (d0k1, d0k2, d0k3)), (gd1_hbm, (d1k1, d1k2, d1k3)))):
        cc = pl.ds(part_no * PIECE_COLS, PIECE_COLS)
        pre.append((grad.at[mine, :], own.at[:, cc]))
        pre.extend((got[k], xrecv.at[k, :, cc]) for k in range(3))
    state = [(gd_hbm.at[mine, :], own.at[:, pl.ds(2 * PIECE_COLS, PIECE_COLS)]),
             (mst_hbm, mst_v), (m_hbm, m_v), (v_hbm, v_v)]
    loads = [pltpu.make_async_copy(src, dst, ld_sem.at[i]) for i, (src, dst) in enumerate(pre + state)]
    for cp in loads:
        cp.start()

    def fetch(items, base=12):
        return [pltpu.make_async_copy(src, dst, ld_sem.at[base + i]) for i, (src, dst) in enumerate(items)]

    top_c, bot_c = pl.ds(0, C_TOP), pl.ds(C_TOP, 768 - C_TOP)
    role_loads = {
        'a': (is_a, fetch([(qa_hbm, sq_a), (ra_hbm, sq_b)])),
        'b': (is_b, fetch([(qb0_hbm, wide_a.at[pl.ds(0, 96), :]), (qb1_hbm, wide_a.at[pl.ds(96, 96), :]),
                           (rb0_hbm, wide_b.at[pl.ds(0, 96), :]), (rb1_hbm, wide_b.at[pl.ds(96, 96), :])])),
        'c': (is_c, fetch([(pc0_hbm, c_a.at[top_c, :]), (pc1_hbm, c_a.at[bot_c, :]),
                           (rc0_hbm, c_b.at[top_c, :]), (rc1_hbm, c_b.at[bot_c, :])])),
        'send0': (is_late, fetch([(pc0_hbm, c_a.at[top_c, :]), (rc0_hbm, c_b.at[top_c, :])], 16)),
        'send1': (is_a, fetch([(pc1_hbm, c_a.at[bot_c, :]), (rc1_hbm, c_b.at[bot_c, :])], 16)),
    }
    for role, copies in role_loads.values():
        @pl.when(role)
        def _():
            for cp in copies:
                cp.start()

    def c_copy(kind):
        rows, where = ((top_c, peers[Y_BIT]), (bot_c, peers[Z_BIT]))[kind]
        return remote(c_a.at[rows, :], sq_b.at[rows, :], c_send.at[kind], c_recv.at[kind], where)

    c_sends = (is_late, is_a)

    def c_add(kind):
        for cp in role_loads['send%d' % kind][1]:
            cp.wait()
        lo, count = ((0, C_TOP), (C_TOP, 768 - C_TOP))[kind]

        def body(i, _):
            rows = pl.ds(pl.multiple_of(lo + i * 16, 16), 16)
            c_a[rows, :] += c_b[rows, :]
            return 0

        lax.fori_loop(0, count // 16, body, 0)

    def spread(terms, groups, tiles):
        def body(g, _):
            rows = pl.ds(pl.multiple_of(g * 8, 8), 8)
            for j in range(tiles):
                cc = pl.ds(128 * j, 128)
                val = terms[0][rows, cc]
                for other in terms[1:]:
                    val = val + other[rows, cc]
                s_v[pl.ds(g * (8 * tiles) + j, 8, stride=tiles), :] = val
            return 0

        lax.fori_loop(0, groups, body, 0)

    for cp in loads[:len(pre)]:
        cp.wait()

    top, bot = pl.ds(0, D_TOP), pl.ds(D_TOP, 192 - D_TOP)
    chain = ((top, top_got, Y_BIT, is_b, is_a), (top, top_got, Z_BIT, is_a, is_c), (top, top_got, Y_BIT, is_c, is_late),
             (bot, bot_got, Z_BIT, is_c, is_a), (bot, bot_got, Y_BIT, is_a, is_b), (bot, bot_got, Z_BIT, is_b, is_late))

    def yz_copy(kind, ch):
        rows, dst, bit = chain[kind][:3]
        return remote(part.at[rows, cols(ch)], dst.at[:, cols(ch)],
                      yz_send.at[kind, ch], yz_recv.at[kind, ch], peers[bit])

    def yz_start(kinds, ch):
        for kind in kinds:
            @pl.when(chain[kind][3])
            def _():
                yz_copy(kind, ch).start()

    def yz_take(kinds, ch):
        for kind in kinds:
            @pl.when(chain[kind][4])
            def _():
                yz_copy(kind, ch).wait_recv()
                got = chain[kind][1]
                base, count = (0, D_TOP) if kind < 3 else (D_TOP, 192 - D_TOP)

                def body(i, _):
                    rows = pl.ds(pl.multiple_of(base + i * 8, 8), 8)
                    part[rows, cols(ch)] += got[pl.ds(pl.multiple_of(i * 8, 8), 8), cols(ch)]
                    return 0

                lax.fori_loop(0, count // 8, body, 0)

    def x_sum(ch):
        if ch >= N_PRE:
            for k in (2, 3, 1):
                xs_copy(k, ch).wait_recv()

        def body(i, _):
            rows = pl.ds(pl.multiple_of(i * 16, 16), 16)
            part[rows, cols(ch)] = ((own[rows, cols(ch)].astype(f32) + xrecv[0, rows, cols(ch)].astype(f32))
                                    + (xrecv[1, rows, cols(ch)].astype(f32) + xrecv[2, rows, cols(ch)].astype(f32)))
            return 0

        lax.fori_loop(0, 12, body, 0)

    def adam():
        def body(i, _):
            rows = pl.ds(pl.multiple_of(i * ADAM_ROWS, ADAM_ROWS), ADAM_ROWS)
            g_sum = s_v[rows, :]
            new_m = BETA_ONE * m_v[rows, :] + (1.0 - BETA_ONE) * g_sum
            new_v = BETA_TWO * v_v[rows, :] + (1.0 - BETA_TWO) * g_sum * g_sum
            m_hat = new_m / (1.0 - BETA_ONE ** STEP)
            v_hat = new_v / (1.0 - BETA_TWO ** STEP)
            new_w = mst_v[rows, :] - LEARN_RATE * m_hat / (jnp.sqrt(v_hat) + ADAM_EPS)
            m_v[rows, :] = new_m
            v_v[rows, :] = new_v
            mst_v[rows, :] = new_w
            w_v[rows, :] = new_w.astype(jnp.bfloat16)
            return 0

        lax.fori_loop(0, SHARD_ROWS // ADAM_ROWS, body, 0)

    def shard_rows(h, r):
        zz = nz if r & Z_BIT else z
        yy = ny if r & Y_BIT else y
        xx = x_peer(2) if r & X_BIT else x
        return pl.ds(pl.multiple_of(((zz * 2 + yy) * 4 + xx) * SHARD_ROWS + h * PIECE_ROWS, 256), PIECE_ROWS)

    def ag_copy(h, r, bit):
        rows = shard_rows(h, r)
        return remote(w_hbm.at[rows, :], w_hbm.at[rows, :], ag_send.at[h, bit.bit_length() - 1, r],
                      ag_recv.at[h, r ^ bit], peers[bit])

    def ag_arrived(h, r):
        rows = shard_rows(h, r)
        bit = ORDERS[h][max(i for i in range(3) if r & ORDERS[h][i])]
        remote(w_hbm.at[rows, :], w_hbm.at[rows, :], ag_send.at[h, 0, r], ag_recv.at[h, r], peers[bit]).wait_recv()

    def dd_copy(h, r):
        rows = shard_rows(h, r)
        return remote(w_hbm.at[rows, :], w_hbm.at[rows, :], dd_send.at[h, r], dd_recv.at[h, r], {'dpx': x_peer(1)})

    def next_bits(h, r):
        last = max([i for i in range(3) if r & ORDERS[h][i]], default=-1)
        return ORDERS[h][last + 1:]

    def hops(step):
        for sub in range(1 << step):
            for h in range(N_PIECE):
                o = ORDERS[h]
                r = o[step] | (o[0] if sub & 1 else 0) | (o[1] if sub & 2 else 0)
                ag_arrived(h, r)
                for bit in next_bits(h, r):
                    ag_copy(h, r, bit).start()
                dd_copy(h, r).start()

    outs = [pltpu.make_async_copy(mst_v, omst_hbm, st_sem.at[0]),
            pltpu.make_async_copy(m_v, om_hbm, st_sem.at[1]),
            pltpu.make_async_copy(v_v, ov_hbm, st_sem.at[2])]

    def own_update():
        adam()
        mine = shard_rows(0, 0)
        rows = pl.ds(mine.start, SHARD_ROWS)
        put = pltpu.make_async_copy(w_v, w_hbm.at[rows, :], st_sem.at[3])
        put.start()
        for cp in outs:
            cp.start()
        put.wait()

    for ch in range(N_PRE):
        x_sum(ch)
        yz_start((0, 3), ch)
    for cp in loads[len(pre):]:
        cp.wait()

    @pl.when(is_late)
    def _():
        c_add(0)
        c_copy(0).start()

    @pl.when(is_a)
    def _():
        c_add(1)

    for name, terms, groups, tiles in (('a', (sq_a, sq_b), 96, 6), ('b', (wide_a, wide_b), 24, 24)):
        role, copies = role_loads[name]

        @pl.when(role)
        def _():
            for cp in copies:
                cp.wait()
            spread(terms, groups, tiles)
            own_update()

    for ch in range(N_PRE):
        yz_take((0, 3), ch)
        yz_start((1, 4), ch)

    @pl.when(is_a)
    def _():
        c_copy(1).start()

    for ch in range(N_PRE, N_CH):
        x_sum(ch)
        yz_start((0, 3), ch)
    for ch in range(N_PRE):
        yz_take((1, 4), ch)
        yz_start((2, 5), ch)
    for ch in range(N_PRE, N_CH):
        yz_take((0, 3), ch)
        yz_start((1, 4), ch)
    for ch in range(N_PRE, N_CH):
        yz_take((1, 4), ch)
        yz_start((2, 5), ch)

    @pl.when(is_late)
    def _():
        for ch in range(N_CH):
            yz_take((2, 5), ch)
        spread((part,), 24, 24)
        own_update()

    @pl.when(is_c)
    def _():
        for cp in role_loads['c'][1]:
            cp.wait()
        for kind in (0, 1):
            c_copy(kind).wait_recv()
        spread((c_a, c_b, sq_b), 96, 6)
        own_update()

    for step in range(3):
        for h in range(N_PIECE):
            ag_copy(h, 0, ORDERS[h][step]).start()
    for h in range(N_PIECE):
        dd_copy(h, 0).start()
    for step in range(3):
        hops(step)

    for h in range(N_PIECE):
        for r in range(8):
            for bit in next_bits(h, r):
                ag_copy(h, r, bit).wait_send()
            dd_copy(h, r).wait()
    for ch in range(N_PRE, N_CH):
        for k in (1, 2, 3):
            xs_copy(k, ch).wait_send()
    for ch in range(N_CH):
        for kind in range(6):
            @pl.when(chain[kind][3])
            def _():
                yz_copy(kind, ch).wait_send()
    for kind in (0, 1):
        @pl.when(c_sends[kind])
        def _():
            c_copy(kind).wait_send()
    for cp in outs:
        cp.wait()


def tail(*args):
    any_spec = pl.BlockSpec(memory_space=pl.ANY)
    f32, bf16 = jnp.float32, jnp.bfloat16
    dma = pltpu.SemaphoreType.DMA
    shard = pltpu.VMEM((SHARD_ROWS, 128), f32)
    square = pltpu.VMEM((768, 768), f32)
    return pl.pallas_call(
        tail_kernel,
        out_shape=(shard, shard, shard, pltpu.VMEM((16 * SHARD_ROWS, 128), bf16)),
        in_specs=[any_spec] * len(args),
        out_specs=[any_spec] * 4,
        scratch_shapes=[
            pltpu.VMEM((192, 3072), bf16), pltpu.VMEM((3, 192, 3072), bf16), pltpu.VMEM((192, 3072), f32),
            pltpu.VMEM((D_TOP, 3072), f32), pltpu.VMEM((192 - D_TOP, 3072), f32), square, square, square, square,
            pltpu.VMEM((192, 3072), f32), pltpu.VMEM((192, 3072), f32),
            shard, shard, shard, shard, pltpu.VMEM((SHARD_ROWS, 128), bf16),
            dma((18,)), dma((4,)), dma((2,)), dma((2,)),
            dma((3, N_CH - N_PRE)), dma((3, N_CH - N_PRE)), dma((6, N_CH)), dma((6, N_CH)),
            dma((N_PIECE, 3, 8)), dma((N_PIECE, 8)), dma((N_PIECE, 8)), dma((N_PIECE, 8)),
        ],
        compiler_params=pltpu.CompilerParams(collective_id=0, has_side_effects=True, vmem_limit_bytes=38 << 20),
        name="tail",
    )(*args)


def slope_product(grad, weight, pre):
    rows, cols, sub = 1024, 1536, 256

    def kernel(grad_ref, weight_ref, pre_ref, out_ref):
        for i in range(rows // sub):
            part = pl.ds(i * sub, sub)
            up = lax.dot_general(grad_ref[part, :], weight_ref[...], (((1,), (1,)), ((), ())),
                                 preferred_element_type=jnp.float32)
            out_ref[part, :] = (up * gelu_slope(pre_ref[part, :].astype(jnp.float32))).astype(jnp.bfloat16)

    tokens, width = grad.shape
    full = weight.shape[0]
    return pl.pallas_call(
        kernel,
        grid=(full // cols, tokens // rows),
        in_specs=[pl.BlockSpec((rows, width), lambda j, i: (i, 0)),
                  pl.BlockSpec((cols, width), lambda j, i: (j, 0)),
                  pl.BlockSpec((rows, cols), lambda j, i: (i, j))],
        out_specs=pl.BlockSpec((rows, cols), lambda j, i: (i, j)),
        out_shape=jax.ShapeDtypeStruct((tokens, full), jnp.bfloat16),
        compiler_params=pltpu.CompilerParams(vmem_limit_bytes=40 << 20),
        cost_estimate=pl.CostEstimate(flops=2 * tokens * width * full, bytes_accessed=4 * tokens * full,
                                      transcendentals=tokens * full),
        name="slope_product",
    )(grad, weight, pre)


def solution(mesh):
    def inner_step(x_one, dy_one, w1_in, w1_out, w2_in, w2_out, master, adam_m, adam_v):
        xi = lax.axis_index('dpx')
        f32, bf16 = jnp.float32, jnp.bfloat16

        def mm(spec, a, b):
            return jnp.einsum(spec, a, b, preferred_element_type=f32)

        z_one = mm('td,df->tf', x_one, w1_in).astype(bf16)
        h_one = gelu_value(z_one.astype(f32)).astype(bf16)
        z_one, h_one = lax.optimization_barrier((z_one, h_one))
        x_two = (x_one.astype(f32) + mm('tf,fd->td', h_one, w1_out)).astype(bf16)
        z_two = mm('td,df->tf', x_two, w2_in).astype(bf16)
        h_two = gelu_value(z_two.astype(f32)).astype(bf16)
        z_two, h_two = lax.optimization_barrier((z_two, h_two))
        g_a = mm('tf,td->fd', h_two, dy_one).astype(bf16)
        x_a = send_x(g_a.reshape(4, 768, 768), xi)
        dz_two = slope_product(dy_one, w2_out, z_two)
        g_b = mm('td,tf->df', x_two, dz_two).astype(bf16)
        x_b = send_x(g_b.reshape(4, 192, 3072), xi)
        p_a = add_x(g_a.reshape(4, 768, 768), xi, x_a)
        dz_two, (p_a,) = after(dz_two, p_a)
        one_a = shift_z(p_a, (0, 1), 0, 0)
        dx_two = (dy_one.astype(f32) + mm('tf,df->td', dz_two, w2_in)).astype(bf16)
        g_c = mm('tf,td->fd', h_one, dx_two).astype(bf16)
        x_c = send_x(g_c.reshape(4, 768, 768), xi)
        p_b = add_x(g_b.reshape(4, 192, 3072), xi, x_b)
        dx_two, (p_b, q_a) = after(dx_two, p_b, p_a + one_a)
        two_a = shift_y(q_a, (0,), 0, 0)
        one_b = send_one(p_b, 0, 1)
        dz_one = slope_product(dx_two, w1_out, z_one)
        dz_one, (qb0, qb1) = after(dz_one, *add_one(one_b))
        two_b = send_two((qb0, qb1), 0, 1)

        def last_piece(grad, i):
            return mm('td,tf->df', x_one, grad[:, i * PIECE_COLS:(i + 1) * PIECE_COLS]).astype(bf16)

        g_d0 = last_piece(dz_one, 0)
        x_d0 = send_x(g_d0.reshape(4, 192, PIECE_COLS), xi)
        p_c = add_x(g_c.reshape(4, 768, 768), xi, x_c)
        dz_one, (p_c,) = after(dz_one, p_c)
        one_c = send_one(p_c, 1, 0, C_TOP)
        g_d1 = last_piece(dz_one, 1)
        x_d1 = send_x(g_d1.reshape(4, 192, PIECE_COLS), xi)
        g_d2 = last_piece(dz_one, 2)
        flat = lambda t: t.reshape(SHARD_ROWS, 128)
        new_master, new_m, new_v, weights = tail(
            g_d0, g_d1, g_d2, *x_d0, *x_d1, q_a, two_a, qb0, qb1, two_b[2], two_b[3], *one_c,
            flat(master), flat(adam_m), flat(adam_v))
        return new_master.reshape(-1), new_m.reshape(-1), new_v.reshape(-1), weights.reshape(-1)

    in_specs = (P(AXES, None), P(AXES, None), P(), P(), P(), P(), P(AXES), P(AXES), P(AXES))
    out_specs = (P(AXES), P(AXES), P(AXES), P())
    return jax.shard_map(inner_step, mesh=mesh, in_specs=in_specs, out_specs=out_specs, check_vma=False)
```
